32 devices in a mesh: dom: 8 (over y, x, core), dim: 4 (over z).
Axes of the slice: x: 2, y: 2, z: 4, core: 2. Of those that a mesh axis runs over, the one named last changes fastest.
Arguments:
- particles: float32 [64, 1024], P('dom', 'dim'), may hold values from -5 to 5
- data_rows: bfloat16 [64, 16, 1024], P('dom', None, 'dim'), may hold values from -0.375 to 0.375
- labels: int32 [64, 16], P('dom'), may hold values from 0 to 1
Outputs:
- updates: float32 [2, 64, 1024], P(None, 'dom', 'dim')
The draws below stay inside these ranges and needn't reach their ends.
All inputs are finite; a program needn't handle non-finite values.
Results may differ from the reference program's by a relative error of at most 0.0003.
Values may be sent and summed in bfloat16 or wider, within the bound.
A program may use at most 64 MiB of HBM per device.

```python
import math
import jax
import jax.numpy as jnp
from jax import lax

D = 1024
R = 16
NEWTON = 2
CG_STEPS = 2
BAND = 1
PARTICLES = 64


def draw_particles(key, part):
    scale_key, value_key = jax.random.split(key, 2)
    spread = jnp.exp(jax.random.uniform(scale_key, (PARTICLES, 1), jnp.float32, math.log(0.4), math.log(1.1)))
    values = jax.random.truncated_normal(value_key, -4.0, 4.0, (PARTICLES, D), jnp.float32)
    return spread * values


def touch_ends(result, key, least, largest):
    shape = result.shape
    spot = [jax.random.randint(jax.random.fold_in(key, axis), (), 0, shape[axis]) for axis in range(len(shape))]
    result = result.at[tuple(spot)].set(least)
    longest = shape.index(max(shape))
    spot[longest] = (spot[longest] + 1) % shape[longest]
    return result.at[tuple(spot)].set(largest)


def shard_levels(rng, dims, shards, least, top_value):
    def one(axis_at, parts):
        heights = jax.random.uniform(jax.random.fold_in(jax.random.fold_in(rng, 6), axis_at), (parts,), jnp.float32, least / len(shards), top_value / len(shards))
        return jnp.repeat(jnp.exp(heights), dims[axis_at] // parts).reshape((-1,) + (1,) * (len(dims) - axis_at - 1))

    loudness = one(*shards[0])
    for cut in shards[1:]:
        loudness = loudness * one(*cut)
    return loudness


def noise(key, dims, width, limit, shards=(), kind=jnp.bfloat16):
    array = jax.random.normal(key, dims, jnp.float32) * width
    if len(shards) > 0:
        array = shard_levels(key, dims, shards, -0.22, 0.18) * array
    return jnp.clip(array, min=-limit, max=limit).astype(kind)


def setup_inputs(seed: int = 0) -> dict:
    keys = jax.random.split(jax.random.key(seed), 4)
    particles = draw_particles(jax.random.fold_in(keys[3], 71), 0)
    data_rows = noise(keys[1], (PARTICLES, R, D), (D // 4) ** -0.5, 0.375, ((0, 8), (2, 4)))
    labels = touch_ends(jax.random.randint(keys[2], (PARTICLES, R), 0, 2), jax.random.fold_in(keys[2], 1), 0, 1).astype(jnp.int32)
    return {"particles": particles, "data_rows": data_rows, "labels": labels}


prior_precision = 0.05
like_weight = 4.0
move_size = 0.5
highest = lax.Precision.HIGHEST


def reference(particles, data_rows, labels):
    factor_rows = data_rows.astype(jnp.float32)
    targets = labels.astype(jnp.float32)
    count = particles.shape[0]
    kernel_scale = 1.0 * BAND * D
    cross_scale = 4.0 / (kernel_scale * kernel_scale)
    current = particles
    outputs = []
    for newton_step in range(NEWTON):
        logits = jnp.einsum("jrd,jd->jr", factor_rows, current, precision=highest)
        probs = jax.nn.sigmoid(logits)
        gradient = -prior_precision * current + like_weight * jnp.einsum("jr,jrd->jd", targets - probs, factor_rows, precision=highest)
        curvature = like_weight * probs * (1.0 - probs)
        squares = jnp.sum(current * current, axis=1)
        inner_rows = jnp.dot(current, current.T, precision=highest)
        distance = squares[:, None] + squares[None, :] - 2.0 * inner_rows
        kernel = jnp.exp(-distance / kernel_scale)
        kernel_sq = kernel * kernel
        kernel_total = jnp.sum(kernel, axis=1)
        square_total = jnp.sum(kernel_sq, axis=1)
        kernel_grad = jnp.dot(kernel, gradient, precision=highest)
        kernel_pos = jnp.dot(kernel, current, precision=highest)
        square_pos = jnp.dot(kernel_sq, current, precision=highest)
        drift = (kernel_grad + (2.0 / kernel_scale) * (current * kernel_total[:, None] - kernel_pos)) / count

        def apply_operator(vectors):
            along_self = jnp.sum(current * vectors, axis=1)
            along_mean = jnp.sum(vectors * square_pos, axis=1)
            projected = jnp.einsum("jrd,id->jri", factor_rows, vectors, precision=highest)
            weighted = projected * curvature[:, :, None] * kernel_sq.T[:, None, :]
            pairs = jnp.einsum("jrd,jri->id", factor_rows, weighted, precision=highest)
            along_pair = jnp.dot(current, vectors.T, precision=highest)
            pairs = pairs + cross_scale * jnp.dot((kernel_sq.T * along_pair).T, current, precision=highest)
            local = prior_precision * square_total[:, None] * vectors + cross_scale * (current * (along_self * square_total - along_mean)[:, None] - along_self[:, None] * square_pos)
            return (pairs + local) / count

        solution = jnp.zeros_like(drift)
        residual = drift
        direction = drift
        norm_now = jnp.sum(residual * residual)
        for solve_step in range(CG_STEPS):
            image = apply_operator(direction)
            alpha = norm_now / jnp.sum(direction * image)
            solution = solution + alpha * direction
            residual = residual - alpha * image
            if solve_step + 1 < CG_STEPS:
                norm_next = jnp.sum(residual * residual)
                direction = residual + (norm_next / norm_now) * direction
                norm_now = norm_next
        outputs.append(solution)
        current = current + move_size * solution
    return jnp.stack(outputs)
```

```python
import functools

import jax
import jax.numpy as jnp
from jax import lax
from jax.experimental import pallas as pl
from jax.experimental.pallas import tpu as pltpu
from jax.sharding import PartitionSpec as P

NEWTON = 2
BAND = 1
LANES = 128

prior_precision = 0.05
like_weight = 4.0
move_size = 0.5
MESH = pl.DeviceIdType.MESH
f32 = jnp.float32
bf16 = jnp.bfloat16


def halves(v):
    high = v.astype(bf16).astype(f32)
    return jnp.concatenate([high, v - high], axis=0).astype(bf16)


def fold(product):
    rows = product.shape[0] // 2
    return product[:rows] + product[rows:]


def dot(a, b):
    return lax.dot_general(a, b, (((1,), (0,)), ((), ())), preferred_element_type=f32)


def dot_t(a, b):
    return lax.dot_general(a, b, (((1,), (1,)), ((), ())), preferred_element_type=f32)


def steps(
    nd, nz, x_ref, a_ref, y_ref, out_ref,
    basis, spread, xbuf, dist, lgt, proj, sums,
    a_send, a_recv, x_send, x_recv, d_send, d_recv, l_send, l_recv, p_send, p_recv, s_send, s_recv,
):
    rows, width = x_ref.shape
    draws = a_ref.shape[0]
    per_row = draws // rows
    count = nd * rows
    wide = dist.shape[-1]
    cols = nd * draws
    scale = 1.0 * BAND * width * nz
    cross = 4.0 / (scale * scale)
    me_dom = lax.axis_index("dom")
    me_dim = lax.axis_index("dim")
    dom_to = [None] + [lax.rem(me_dom + k, nd) for k in range(1, nd)]
    dim_to = [None] + [lax.rem(me_dim + k, nz) for k in range(1, nz)]

    def send_all(axis, src, dst, send, recv):
        to = dom_to if axis == "dom" else dim_to
        copies = []
        for k in range(1, len(to)):
            copy = pltpu.make_async_remote_copy(
                src_ref=src, dst_ref=dst(k), send_sem=send(k), recv_sem=recv(k),
                device_id={axis: to[k]}, device_id_type=MESH,
            )
            copy.start()
            copies.append(copy)
        return copies

    barrier = pltpu.get_barrier_semaphore()
    for k in range(1, nd):
        pl.semaphore_signal(barrier, inc=1, device_id={"dom": dom_to[k]}, device_id_type=MESH)
    for k in range(1, nz):
        pl.semaphore_signal(barrier, inc=1, device_id={"dim": dim_to[k]}, device_id_type=MESH)

    lane_of = lax.broadcasted_iota(jnp.int32, (rows, draws), 1) // per_row
    row_of = lax.broadcasted_iota(jnp.int32, (rows, draws), 0)
    own_block = lane_of == row_of

    def flat(values):
        return jnp.sum(jnp.where(own_block, values, 0.0), axis=0, keepdims=True)

    basis[0:draws, :] = a_ref[...]
    tile = lax.broadcasted_iota(jnp.int32, (per_row, draws), 1) % per_row
    tile = (tile == lax.broadcasted_iota(jnp.int32, (per_row, draws), 0)).astype(f32).astype(bf16)
    labels = flat(dot(y_ref[...].astype(f32).astype(bf16), tile))
    current = x_ref[...]
    pending = []
    a_copies = []
    first_eight = lax.broadcasted_iota(jnp.int32, (rows, wide), 1)
    own_pair = first_eight == lax.broadcasted_iota(jnp.int32, (rows, wide), 0)
    lane = lax.broadcasted_iota(jnp.int32, (rows, LANES), 1)

    for t in range(NEWTON):
        xbuf[t, 0, :, 0:width] = current
        own_logits = flat(fold(dot_t(halves(current), a_ref[...])))
        xbuf[t, 0, 0:1, width:] = own_logits
        xbuf[t, 0, 1:2, width:] = labels
        if t == 0:
            pl.semaphore_wait(barrier, nd - 1 + nz - 1)
        copies = send_all(
            "dom", xbuf.at[t, 0], lambda k: xbuf.at[t, k], lambda k: x_send.at[t, k], lambda k: x_recv.at[t, k]
        )
        pending += copies
        if t == 0:
            a_copies = send_all(
                "dom", a_ref, lambda k: basis.at[pl.ds(k * draws, draws), :],
                lambda k: a_send.at[k], lambda k: a_recv.at[k],
            )
            pending += a_copies
            spread_col = lax.broadcasted_iota(jnp.int32, spread.shape, 1) // per_row
            spread_row = lax.broadcasted_iota(jnp.int32, spread.shape, 0)
            spread[...] = (spread_col == spread_row).astype(f32).astype(bf16)
        for copy in copies:
            copy.wait_recv()
        everyone = xbuf[t, :, :, 0:width].reshape(count, width)
        pieces = halves(everyone)
        basis[cols:, :] = pieces
        for k in range(nd):
            lgt[t, 0, k : k + 1, :] = xbuf[t, k, 0:1, width:]
        inner = fold(dot_t(halves(current), pieces))
        inner = inner[:, :count] + inner[:, count:]
        sq_all = dot_t(jnp.ones((rows, width), bf16), halves(everyone * everyone))
        sq_all = sq_all[:, :count] + sq_all[:, count:]
        sq_own = jnp.sum(current * current, axis=1, keepdims=True)
        dist[t, 0, :, 0:count] = sq_own + sq_all - 2.0 * inner
        if wide > count:
            dist[t, 0, :, count:] = jnp.zeros((rows, wide - count), f32)
        c1 = send_all("dim", dist.at[t, 0], lambda k: dist.at[t, k], lambda k: d_send.at[t, k], lambda k: d_recv.at[t, k])
        c2 = send_all("dim", lgt.at[t, 0], lambda k: lgt.at[t, k], lambda k: l_send.at[t, k], lambda k: l_recv.at[t, k])
        pending += c1 + c2
        for copy in c1 + c2:
            copy.wait_recv()
        distance = functools.reduce(jnp.add, [dist[t, k] for k in range(nz)])
        logits = functools.reduce(jnp.add, [lgt[t, k] for k in range(nz)])
        prob = 1.0 / (1.0 + jnp.exp(-logits))
        curve = like_weight * prob * (1.0 - prob)
        real = first_eight < count
        kernel = jnp.where(real, jnp.exp(-distance / scale), 0.0)
        kernel_sq = kernel * kernel
        total = jnp.sum(kernel, axis=1, keepdims=True)
        total_sq = jnp.sum(kernel_sq, axis=1, keepdims=True)
        both = jnp.concatenate([kernel, kernel_sq], axis=0)[:, :count]
        wider = fold(dot(halves(both), spread[...]))
        kernel_wide, kernel_sq_wide = wider[:rows], wider[rows:]
        weight, drive = [], []
        for k in range(nd):
            part = slice(k * draws, (k + 1) * draws)
            gap = like_weight * (xbuf[t, k, 1:2, width:] - prob[k : k + 1])
            drive.append(kernel_wide[:, part] * gap)
            weight.append(kernel_sq_wide[:, part] * curve[k : k + 1])
        weight = jnp.concatenate(weight, axis=1)
        drive = jnp.concatenate(drive, axis=1)
        if t == 0:
            for copy in a_copies:
                copy.wait_recv()
        pull = (-prior_precision - 2.0 / scale) * kernel[:, :count]

        def back(on_rows, on_x):
            return fold(dot(halves(jnp.concatenate([on_rows, on_x, on_x], axis=1)), basis[...]))

        def ahead(vectors, slot):
            out = fold(dot_t(halves(vectors), basis[...]))
            proj[t, slot, 0, :, 0:cols] = out[:, :cols]
            proj[t, slot, 0, :, cols : cols + count] = out[:, cols : cols + count] + out[:, cols + count :]
            if wide > count:
                proj[t, slot, 0, :, cols + count : cols + wide] = jnp.zeros((rows, wide - count), f32)

        def exchange(slot):
            done = send_all(
                "dim", proj.at[t, slot, 0], lambda k: proj.at[t, slot, k],
                lambda k: p_send.at[t, slot, k], lambda k: p_recv.at[t, slot, k],
            )
            for copy in done:
                copy.wait_recv()
            return done, functools.reduce(jnp.add, [proj[t, slot, k] for k in range(nz)])

        def own_dots(along):
            return jnp.sum(jnp.where(own_pair, along, 0.0), axis=1, keepdims=True)

        drift = (back(drive, pull) + (2.0 / scale) * total * current) / count
        ahead(drift, 0)
        proj[t, 0, 0, :, cols + wide :] = jnp.zeros((rows, LANES), f32)
        done, seen = exchange(0)
        pending += done
        along = seen[:, cols : cols + wide]
        on_x = cross * kernel_sq * (along - own_dots(along))
        image = back(weight * seen[:, :cols], on_x[:, :count])
        image = image + prior_precision * total_sq * drift - jnp.sum(on_x, axis=1, keepdims=True) * current
        image = image / count
        ahead(image, 1)
        image_sq = jnp.sum(image * image, axis=1, keepdims=True)
        marks = jnp.where(lane == 0, jnp.sum(drift * drift, axis=1, keepdims=True), 0.0)
        marks = jnp.where(lane == 1, jnp.sum(drift * image, axis=1, keepdims=True), marks)
        marks = jnp.where(lane == 2, image_sq, marks)
        marks = jnp.where(lane == 3, prior_precision * total_sq * image_sq, marks)
        proj[t, 1, 0, :, cols + wide :] = marks
        done, seen = exchange(1)
        pending += done
        along = seen[:, cols : cols + wide]
        gap = along - own_dots(along)
        bent = jnp.sum(weight * seen[:, :cols] * seen[:, :cols], axis=1, keepdims=True)
        bent = bent + cross * jnp.sum(kernel_sq * gap * gap, axis=1, keepdims=True)
        marks = seen[:, cols + wide :]
        sums[t, 0] = marks + jnp.where(lane == 3, bent, 0.0)
        copies = send_all(
            "dom", sums.at[t, 0], lambda k: sums.at[t, k], lambda k: s_send.at[t, k], lambda k: s_recv.at[t, k]
        )
        pending += copies
        for copy in copies:
            copy.wait_recv()
        marks = functools.reduce(jnp.add, [sums[t, k] for k in range(nd)])
        marks = jnp.sum(marks, axis=0, keepdims=True)
        first = lax.broadcasted_iota(jnp.int32, (1, LANES), 1)
        norm, curve_total, image_square, bent = [
            jnp.sum(jnp.where(first == k, marks, 0.0), axis=1, keepdims=True) for k in range(4)
        ]
        bent = bent / count
        alpha = norm / curve_total
        norm_next = norm - 2.0 * alpha * curve_total + alpha * alpha * image_square
        keep = 1.0 + norm_next / norm
        curve_next = keep * keep * curve_total - 2.0 * keep * alpha * image_square + alpha * alpha * bent
        alpha_next = norm_next / curve_next
        update = (alpha + alpha_next * keep) * drift - (alpha_next * alpha) * image
        out_ref[t] = update
        current = current + move_size * update
    for copy in pending:
        copy.wait_send()


def solution(mesh):
    nd, nz = mesh.shape["dom"], mesh.shape["dim"]

    def per_device(particles, data_rows, labels):
        rows, width = particles.shape
        draws = data_rows.shape[0] * data_rows.shape[1]
        count = nd * rows
        wide = -(-count // LANES) * LANES
        cols = nd * draws
        dma = pltpu.SemaphoreType.DMA
        pairs = [(nd,), (NEWTON, nd), (NEWTON, nz), (NEWTON, nz), (NEWTON, 2, nz), (NEWTON, nd)]
        return pl.pallas_call(
            functools.partial(steps, nd, nz),
            out_shape=jax.ShapeDtypeStruct((NEWTON, rows, width), f32),
            in_specs=[pl.BlockSpec(memory_space=pltpu.VMEM)] * 3,
            out_specs=pl.BlockSpec(memory_space=pltpu.VMEM),
            scratch_shapes=[
                pltpu.VMEM((cols + 2 * count, width), bf16),
                pltpu.VMEM((count, cols), bf16),
                pltpu.VMEM((NEWTON, nd, rows, width + draws), f32),
                pltpu.VMEM((NEWTON, nz, rows, wide), f32),
                pltpu.VMEM((NEWTON, nz, nd, draws), f32),
                pltpu.VMEM((NEWTON, 2, nz, rows, cols + wide + LANES), f32),
                pltpu.VMEM((NEWTON, nd, rows, LANES), f32),
            ]
            + [dma(shape) for shape in pairs for _ in range(2)],
            compiler_params=pltpu.CompilerParams(collective_id=0, has_side_effects=True),
        )(particles, data_rows.reshape(draws, width), labels)

    placed = (P("dom", "dim"), P("dom", None, "dim"), P("dom", None))
    return jax.shard_map(
        per_device, mesh=mesh, in_specs=placed, out_specs=P(None, "dom", "dim"), check_vma=False
    )
```

```python
import functools

import jax
import jax.numpy as jnp
from jax import lax
from jax.experimental import pallas as pl
from jax.experimental.pallas import tpu as pltpu
from jax.sharding import PartitionSpec as P

NEWTON = 2
BAND = 1
LANES = 128

prior_precision = 0.05
like_weight = 4.0
move_size = 0.5
MESH = pl.DeviceIdType.MESH
f32 = jnp.float32
bf16 = jnp.bfloat16


def halves(v):
    high = v.astype(bf16).astype(f32)
    return jnp.concatenate([high, v - high], axis=0).astype(bf16)


def fold(product):
    rows = product.shape[0] // 2
    return product[:rows] + product[rows:]


def dot(a, b):
    return lax.dot_general(a, b, (((1,), (0,)), ((), ())), preferred_element_type=f32)


def dot_t(a, b):
    return lax.dot_general(a, b, (((1,), (1,)), ((), ())), preferred_element_type=f32)


def steps(
    nd, nz, x_ref, a_ref, y_ref, out_ref,
    basis, spread, xbuf, dist, lgt, proj, rough, marked, sums,
    a_send, a_recv, x_send, x_recv, d_send, d_recv, l_send, l_recv, p_send, p_recv,
    r_send, r_recv, m_send, m_recv, s_send, s_recv,
):
    rows, width = x_ref.shape
    draws = a_ref.shape[0]
    per_row = draws // rows
    count = nd * rows
    wide = dist.shape[-1]
    cols = nd * draws
    scale = 1.0 * BAND * width * nz
    cross = 4.0 / (scale * scale)
    me_dom = lax.axis_index("dom")
    me_dim = lax.axis_index("dim")
    chips = nd // 2
    chip, core = me_dom // 2, me_dom % 2
    dom_to = [((chip + m // 2) % chips) * 2 + (core + m) % 2 for m in range(nd)]
    upper = (me_dim * 2) // nz

    def dom_copy(m, src, dst, send, recv):
        return pltpu.make_async_remote_copy(
            src_ref=src, dst_ref=dst(m), send_sem=send(m), recv_sem=recv(m),
            device_id={"dom": dom_to[m]}, device_id_type=MESH,
        )

    def send_dom(*what):
        copies = [dom_copy(m, *what) for m in range(1, nd)]
        for copy in copies:
            copy.start()
        return copies

    def send_dim(src, dst, send, recv):
        def one(k):
            return pltpu.make_async_remote_copy(
                src_ref=src, dst_ref=dst(k), send_sem=send(k), recv_sem=recv(k),
                device_id={"dim": lax.rem(me_dim + k, nz)}, device_id_type=MESH,
            )

        for k in range(1, nz):
            one(upper * k + (1 - upper) * (nz - k)).start()
        return [one(k) for k in range(1, nz)]

    barrier = pltpu.get_barrier_semaphore()
    for k in range(1, nd):
        pl.semaphore_signal(barrier, inc=1, device_id={"dom": dom_to[k]}, device_id_type=MESH)
    for k in range(1, nz):
        pl.semaphore_signal(barrier, inc=1, device_id={"dim": lax.rem(me_dim + k, nz)}, device_id_type=MESH)

    lane_of = lax.broadcasted_iota(jnp.int32, (rows, draws), 1) // per_row
    row_of = lax.broadcasted_iota(jnp.int32, (rows, draws), 0)
    own_block = lane_of == row_of

    def flat(values):
        return jnp.sum(jnp.where(own_block, values, 0.0), axis=0, keepdims=True)

    basis[0:draws, :] = a_ref[...]
    tile = lax.broadcasted_iota(jnp.int32, (per_row, draws), 1) % per_row
    tile = (tile == lax.broadcasted_iota(jnp.int32, (per_row, draws), 0)).astype(f32).astype(bf16)
    labels = flat(dot(y_ref[...].astype(f32).astype(bf16), tile))
    current = x_ref[...]
    pending = []
    first_eight = lax.broadcasted_iota(jnp.int32, (rows, wide), 1)
    own_pair = first_eight == lax.broadcasted_iota(jnp.int32, (rows, wide), 0)
    lane = lax.broadcasted_iota(jnp.int32, (rows, LANES), 1)

    for t in range(NEWTON):
        xbuf[t, 0, :, 0:width] = current
        own_logits = flat(fold(dot_t(halves(current), a_ref[...])))
        xbuf[t, 0, 0:1, width:] = own_logits
        xbuf[t, 0, 1:2, width:] = labels
        if t == 0:
            pl.semaphore_wait(barrier, nd - 1 + nz - 1)
        copies = send_dom(
            xbuf.at[t, 0], lambda k: xbuf.at[t, k], lambda k: x_send.at[t, k], lambda k: x_recv.at[t, k]
        )
        pending += copies
        if t == 0:
            a_parts = (
                lambda k: basis.at[pl.ds(k * draws, draws), :], lambda k: a_send.at[k], lambda k: a_recv.at[k],
            )
            a_far = [dom_copy(m, a_ref, *a_parts) for m in range(2, nd, 2)]
            a_near = [dom_copy(1, a_ref, *a_parts)]
            for copy in a_far + a_near:
                copy.start()
            spread_col = lax.broadcasted_iota(jnp.int32, spread.shape, 1) // per_row
            spread_row = lax.broadcasted_iota(jnp.int32, spread.shape, 0)
            spread[...] = (spread_col == spread_row).astype(f32).astype(bf16)
        for copy in copies:
            copy.wait_recv()
        everyone = xbuf[t, :, :, 0:width].reshape(count, width)
        pieces = halves(everyone)
        basis[cols:, :] = pieces
        for k in range(nd):
            lgt[t, 0, k : k + 1, :] = xbuf[t, k, 0:1, width:]
        inner = fold(dot_t(halves(current), pieces))
        inner = inner[:, :count] + inner[:, count:]
        sq_all = dot_t(jnp.ones((rows, width), bf16), halves(everyone * everyone))
        sq_all = sq_all[:, :count] + sq_all[:, count:]
        sq_own = jnp.sum(current * current, axis=1, keepdims=True)
        dist[t, 0, :, 0:count] = sq_own + sq_all - 2.0 * inner
        if wide > count:
            dist[t, 0, :, count:] = jnp.zeros((rows, wide - count), f32)
        c1 = send_dim(dist.at[t, 0], lambda k: dist.at[t, k], lambda k: d_send.at[t, k], lambda k: d_recv.at[t, k])
        c2 = send_dim(lgt.at[t, 0], lambda k: lgt.at[t, k], lambda k: l_send.at[t, k], lambda k: l_recv.at[t, k])
        pending += c1 + c2
        if t == 0:
            for m, copy in zip(range(2, nd, 2), a_far):
                copy.wait_recv()
                part = basis.at[pl.ds(m * draws, draws), :]
                on = pltpu.make_async_remote_copy(
                    src_ref=part, dst_ref=basis.at[pl.ds((m + 1) * draws, draws), :],
                    send_sem=a_send.at[m + 1], recv_sem=a_recv.at[m + 1],
                    device_id={"dom": dom_to[1]}, device_id_type=MESH,
                )
                on.start()
                a_near.append(on)
            pending += a_far + a_near
        for copy in c1 + c2:
            copy.wait_recv()
        distance = functools.reduce(jnp.add, [dist[t, k] for k in range(nz)])
        logits = functools.reduce(jnp.add, [lgt[t, k] for k in range(nz)])
        prob = 1.0 / (1.0 + jnp.exp(-logits))
        curve = like_weight * prob * (1.0 - prob)
        real = first_eight < count
        kernel = jnp.where(real, jnp.exp(-distance / scale), 0.0)
        kernel_sq = kernel * kernel
        total = jnp.sum(kernel, axis=1, keepdims=True)
        total_sq = jnp.sum(kernel_sq, axis=1, keepdims=True)
        both = jnp.concatenate([kernel, kernel_sq], axis=0)[:, :count]
        wider = fold(dot(halves(both), spread[...]))
        kernel_wide, kernel_sq_wide = wider[:rows], wider[rows:]
        weight, drive = [], []
        for k in range(nd):
            part = slice(k * draws, (k + 1) * draws)
            gap = like_weight * (xbuf[t, k, 1:2, width:] - prob[k : k + 1])
            drive.append(kernel_wide[:, part] * gap)
            weight.append(kernel_sq_wide[:, part] * curve[k : k + 1])
        weight = jnp.concatenate(weight, axis=1)
        drive = jnp.concatenate(drive, axis=1)
        if t == 0:
            for copy in a_near:
                copy.wait_recv()
        pull = (-prior_precision - 2.0 / scale) * kernel[:, :count]

        def back(on_rows, on_x):
            return fold(dot(halves(jnp.concatenate([on_rows, on_x, on_x], axis=1)), basis[...]))

        def ahead(vectors):
            out = fold(dot_t(halves(vectors), basis[...]))
            parts = [out[:, :cols], out[:, cols : cols + count] + out[:, cols + count :]]
            if wide > count:
                parts.append(jnp.zeros((rows, wide - count), f32))
            return jnp.concatenate(parts, axis=1)

        def own_dots(along):
            return jnp.sum(jnp.where(own_pair, along, 0.0), axis=1, keepdims=True)

        drift = (back(drive, pull) + (2.0 / scale) * total * current) / count
        proj[t, 0] = ahead(drift)
        copies = send_dim(proj.at[t, 0], lambda k: proj.at[t, k], lambda k: p_send.at[t, k], lambda k: p_recv.at[t, k])
        pending += copies
        for copy in copies:
            copy.wait_recv()
        seen = functools.reduce(jnp.add, [proj[t, k] for k in range(nz)])
        along = seen[:, cols : cols + wide]
        on_x = cross * kernel_sq * (along - own_dots(along))
        image = back(weight * seen[:, :cols], on_x[:, :count])
        image = image + prior_precision * total_sq * drift - jnp.sum(on_x, axis=1, keepdims=True) * current
        image = image / count
        exact = ahead(image)
        rough[t, 0] = exact.astype(bf16)
        c1 = send_dim(rough.at[t, 0], lambda k: rough.at[t, k], lambda k: r_send.at[t, k], lambda k: r_recv.at[t, k])
        image_sq = jnp.sum(image * image, axis=1, keepdims=True)
        marks = jnp.where(lane == 0, jnp.sum(drift * drift, axis=1, keepdims=True), 0.0)
        marks = jnp.where(lane == 1, jnp.sum(drift * image, axis=1, keepdims=True), marks)
        marks = jnp.where(lane == 2, image_sq, marks)
        marks = jnp.where(lane == 3, prior_precision * total_sq * image_sq, marks)
        marked[t, 0] = marks
        c2 = send_dim(marked.at[t, 0], lambda k: marked.at[t, k], lambda k: m_send.at[t, k], lambda k: m_recv.at[t, k])
        pending += c1 + c2
        for copy in c1 + c2:
            copy.wait_recv()
        seen = functools.reduce(jnp.add, [rough[t, k].astype(f32) for k in range(1, nz)], exact)
        along = seen[:, cols : cols + wide]
        gap = along - own_dots(along)
        bent = jnp.sum(weight * seen[:, :cols] * seen[:, :cols], axis=1, keepdims=True)
        bent = bent + cross * jnp.sum(kernel_sq * gap * gap, axis=1, keepdims=True)
        marks = functools.reduce(jnp.add, [marked[t, k] for k in range(nz)])
        sums[t, 0] = marks + jnp.where(lane == 3, bent, 0.0)
        copies = send_dom(
            sums.at[t, 0], lambda k: sums.at[t, k], lambda k: s_send.at[t, k], lambda k: s_recv.at[t, k]
        )
        pending += copies
        for copy in copies:
            copy.wait_recv()
        marks = functools.reduce(jnp.add, [sums[t, k] for k in range(nd)])
        marks = jnp.sum(marks, axis=0, keepdims=True)
        first = lax.broadcasted_iota(jnp.int32, (1, LANES), 1)
        norm, curve_total, image_square, bent = [
            jnp.sum(jnp.where(first == k, marks, 0.0), axis=1, keepdims=True) for k in range(4)
        ]
        bent = bent / count
        alpha = norm / curve_total
        norm_next = norm - 2.0 * alpha * curve_total + alpha * alpha * image_square
        keep = 1.0 + norm_next / norm
        curve_next = keep * keep * curve_total - 2.0 * keep * alpha * image_square + alpha * alpha * bent
        alpha_next = norm_next / curve_next
        update = (alpha + alpha_next * keep) * drift - (alpha_next * alpha) * image
        out_ref[t] = update
        current = current + move_size * update
    for copy in pending:
        copy.wait_send()


def solution(mesh):
    nd, nz = mesh.shape["dom"], mesh.shape["dim"]

    def per_device(particles, data_rows, labels):
        rows, width = particles.shape
        draws = data_rows.shape[0] * data_rows.shape[1]
        count = nd * rows
        wide = -(-count // LANES) * LANES
        cols = nd * draws
        dma = pltpu.SemaphoreType.DMA
        over_dom, over_dim = (NEWTON, nd), (NEWTON, nz)
        pairs = [(nd,), over_dom] + [over_dim] * 5 + [over_dom]
        return pl.pallas_call(
            functools.partial(steps, nd, nz),
            out_shape=jax.ShapeDtypeStruct((NEWTON, rows, width), f32),
            in_specs=[pl.BlockSpec(memory_space=pltpu.VMEM)] * 3,
            out_specs=pl.BlockSpec(memory_space=pltpu.VMEM),
            scratch_shapes=[
                pltpu.VMEM((cols + 2 * count, width), bf16),
                pltpu.VMEM((count, cols), bf16),
                pltpu.VMEM((NEWTON, nd, rows, width + draws), f32),
                pltpu.VMEM((NEWTON, nz, rows, wide), f32),
                pltpu.VMEM((NEWTON, nz, nd, draws), f32),
                pltpu.VMEM((NEWTON, nz, rows, cols + wide), f32),
                pltpu.VMEM((NEWTON, nz, rows, cols + wide), bf16),
                pltpu.VMEM((NEWTON, nz, rows, LANES), f32),
                pltpu.VMEM((NEWTON, nd, rows, LANES), f32),
            ]
            + [dma(shape) for shape in pairs for _ in range(2)],
            compiler_params=pltpu.CompilerParams(collective_id=0, has_side_effects=True),
        )(particles, data_rows.reshape(draws, width), labels)

    placed = (P("dom", "dim"), P("dom", None, "dim"), P("dom", None))
    return jax.shard_map(
        per_device, mesh=mesh, in_specs=placed, out_specs=P(None, "dom", "dim"), check_vma=False
    )
```

```python
import functools

import jax
import jax.numpy as jnp
from jax import lax
from jax.experimental import pallas as pl
from jax.experimental.pallas import tpu as pltpu
from jax.sharding import PartitionSpec as P

NEWTON = 2
BAND = 1
LANES = 128

prior_precision = 0.05
like_weight = 4.0
move_size = 0.5
MESH = pl.DeviceIdType.MESH
f32 = jnp.float32
bf16 = jnp.bfloat16


def halves(v):
    high = v.astype(bf16).astype(f32)
    return jnp.concatenate([high, v - high], axis=0).astype(bf16)


def fold(product):
    rows = product.shape[0] // 2
    return product[:rows] + product[rows:]


def dot(a, b):
    return lax.dot_general(a, b, (((1,), (0,)), ((), ())), preferred_element_type=f32)


def dot_t(a, b):
    return lax.dot_general(a, b, (((1,), (1,)), ((), ())), preferred_element_type=f32)


def steps(
    nd, nz, x_ref, a_ref, y_ref, out_ref,
    basis, spread, xbuf, dist, lgt, proj, rough, marked, sums, moves, cross_terms,
    a_send, a_recv, x_send, x_recv, d_send, d_recv, l_send, l_recv, p_send, p_recv,
    r_send, r_recv, m_send, m_recv, s_send, s_recv,
    b_send, b_recv, h_send, h_recv, g_send, g_recv,
):
    rows, width = x_ref.shape
    draws = a_ref.shape[0]
    per_row = draws // rows
    count = nd * rows
    wide = dist.shape[-1]
    cols = nd * draws
    scale = 1.0 * BAND * width * nz
    cross = 4.0 / (scale * scale)
    me_dom = lax.axis_index("dom")
    me_dim = lax.axis_index("dim")
    chips = nd // 2
    chip, core = me_dom // 2, me_dom % 2
    dom_to = [((chip + m // 2) % chips) * 2 + (core + m) % 2 for m in range(nd)]
    upper = (me_dim * 2) // nz

    def dom_copy(m, src, dst, send, recv):
        return pltpu.make_async_remote_copy(
            src_ref=src, dst_ref=dst(m), send_sem=send(m), recv_sem=recv(m),
            device_id={"dom": dom_to[m]}, device_id_type=MESH,
        )

    def send_dom(*what):
        copies = [dom_copy(m, *what) for m in range(1, nd)]
        for copy in copies:
            copy.start()
        return copies

    def send_dim(src, dst, send, recv):
        def one(k):
            return pltpu.make_async_remote_copy(
                src_ref=src, dst_ref=dst(k), send_sem=send(k), recv_sem=recv(k),
                device_id={"dim": lax.rem(me_dim + k, nz)}, device_id_type=MESH,
            )

        for k in range(1, nz):
            one(upper * k + (1 - upper) * (nz - k)).start()
        return [one(k) for k in range(1, nz)]

    barrier = pltpu.get_barrier_semaphore()
    for k in range(1, nd):
        pl.semaphore_signal(barrier, inc=1, device_id={"dom": dom_to[k]}, device_id_type=MESH)
    for k in range(1, nz):
        pl.semaphore_signal(barrier, inc=1, device_id={"dim": lax.rem(me_dim + k, nz)}, device_id_type=MESH)

    lane_of = lax.broadcasted_iota(jnp.int32, (rows, draws), 1) // per_row
    row_of = lax.broadcasted_iota(jnp.int32, (rows, draws), 0)
    own_block = lane_of == row_of

    def flat(values):
        return jnp.sum(jnp.where(own_block, values, 0.0), axis=0, keepdims=True)

    basis[0:draws, :] = a_ref[...]
    tile = lax.broadcasted_iota(jnp.int32, (per_row, draws), 1) % per_row
    tile = (tile == lax.broadcasted_iota(jnp.int32, (per_row, draws), 0)).astype(f32).astype(bf16)
    labels = flat(dot(y_ref[...].astype(f32).astype(bf16), tile))
    current = x_ref[...]
    pending = []
    first_eight = lax.broadcasted_iota(jnp.int32, (rows, count), 1)
    own_pair = first_eight == lax.broadcasted_iota(jnp.int32, (rows, count), 0)
    lane = lax.broadcasted_iota(jnp.int32, (rows, LANES), 1)

    def paired(product):
        return product[:, : product.shape[1] // 2] + product[:, product.shape[1] // 2 :]

    def column_sums(values):
        return paired(dot_t(jnp.ones((rows, width), bf16), halves(values)))

    def row_sums(values):
        return jnp.sum(values, axis=1, keepdims=True)

    xbuf[0, :, 0:width] = current
    xbuf[0, 0:1, width:] = flat(fold(dot_t(halves(current), a_ref[...])))
    xbuf[0, 1:2, width:] = labels
    pl.semaphore_wait(barrier, nd - 1 + nz - 1)
    copies = send_dom(xbuf.at[0], lambda k: xbuf.at[k], lambda k: x_send.at[k], lambda k: x_recv.at[k])
    pending += copies
    a_parts = (
        lambda k: basis.at[pl.ds(k * draws, draws), :], lambda k: a_send.at[k], lambda k: a_recv.at[k],
    )
    a_far = [dom_copy(m, a_ref, *a_parts) for m in range(2, nd, 2)]
    a_near = [dom_copy(1, a_ref, *a_parts)]
    for copy in a_far + a_near:
        copy.start()
    spread_col = lax.broadcasted_iota(jnp.int32, spread.shape, 1) // per_row
    spread_row = lax.broadcasted_iota(jnp.int32, spread.shape, 0)
    spread[...] = (spread_col == spread_row).astype(f32).astype(bf16)
    for copy in copies:
        copy.wait_recv()
    everyone = xbuf[:, :, 0:width].reshape(count, width)
    pieces = halves(everyone)
    basis[cols:, :] = pieces
    for k in range(nd):
        lgt[0, k : k + 1, :] = xbuf[k, 0:1, width:]
    inner = paired(fold(dot_t(halves(current), pieces)))
    dist[0, :, 0:count] = row_sums(current * current) + column_sums(everyone * everyone) - 2.0 * inner
    if wide > count:
        dist[0, :, count:] = jnp.zeros((rows, wide - count), f32)
    c1 = send_dim(dist.at[0], lambda k: dist.at[k], lambda k: d_send.at[k], lambda k: d_recv.at[k])
    c2 = send_dim(lgt.at[0], lambda k: lgt.at[k], lambda k: l_send.at[k], lambda k: l_recv.at[k])
    pending += c1 + c2
    for m, copy in zip(range(2, nd, 2), a_far):
        copy.wait_recv()
        on = pltpu.make_async_remote_copy(
            src_ref=basis.at[pl.ds(m * draws, draws), :], dst_ref=basis.at[pl.ds((m + 1) * draws, draws), :],
            send_sem=a_send.at[m + 1], recv_sem=a_recv.at[m + 1],
            device_id={"dom": dom_to[1]}, device_id_type=MESH,
        )
        on.start()
        a_near.append(on)
    pending += a_far + a_near
    for copy in c1 + c2:
        copy.wait_recv()
    distance = functools.reduce(jnp.add, [dist[k] for k in range(nz)])[:, :count]
    logits = functools.reduce(jnp.add, [lgt[k] for k in range(nz)])

    for t in range(NEWTON):
        last = t + 1 == NEWTON
        prob = 1.0 / (1.0 + jnp.exp(-logits))
        curve = like_weight * prob * (1.0 - prob)
        kernel = jnp.exp(-distance / scale)
        kernel_sq = kernel * kernel
        total = jnp.sum(kernel, axis=1, keepdims=True)
        total_sq = jnp.sum(kernel_sq, axis=1, keepdims=True)
        both = jnp.concatenate([kernel, kernel_sq], axis=0)
        wider = fold(dot(halves(both), spread[...]))
        kernel_wide, kernel_sq_wide = wider[:rows], wider[rows:]
        weight, drive = [], []
        for k in range(nd):
            part = slice(k * draws, (k + 1) * draws)
            gap = like_weight * (xbuf[k, 1:2, width:] - prob[k : k + 1])
            drive.append(kernel_wide[:, part] * gap)
            weight.append(kernel_sq_wide[:, part] * curve[k : k + 1])
        weight = jnp.concatenate(weight, axis=1)
        drive = jnp.concatenate(drive, axis=1)
        if t == 0:
            for copy in a_near:
                copy.wait_recv()
        pull = (-prior_precision - 2.0 / scale) * kernel

        def back(on_rows, on_x):
            return fold(dot(halves(jnp.concatenate([on_rows, on_x, on_x], axis=1)), basis[...]))

        def ahead(vectors):
            out = fold(dot_t(halves(vectors), basis[...]))
            parts = [out[:, :cols], out[:, cols : cols + count] + out[:, cols + count :]]
            if wide > count:
                parts.append(jnp.zeros((rows, wide - count), f32))
            return jnp.concatenate(parts, axis=1)

        def own_dots(along):
            return jnp.sum(jnp.where(own_pair, along, 0.0), axis=1, keepdims=True)

        drift = (back(drive, pull) + (2.0 / scale) * total * current) / count
        proj[t, 0] = ahead(drift)
        copies = send_dim(proj.at[t, 0], lambda k: proj.at[t, k], lambda k: p_send.at[t, k], lambda k: p_recv.at[t, k])
        pending += copies
        if not last:
            moves[t, 0, 0] = drift
            b_copies = send_dom(
                moves.at[t, 0, 0], lambda k: moves.at[t, 0, k], lambda k: b_send.at[t, k], lambda k: b_recv.at[t, k]
            )
            pending += b_copies
        for copy in copies:
            copy.wait_recv()
        seen = functools.reduce(jnp.add, [proj[t, k] for k in range(nz)])
        drift_logits = flat(seen[:, :draws])
        along = seen[:, cols : cols + count]
        on_x = cross * kernel_sq * (along - own_dots(along))
        image = back(weight * seen[:, :cols], on_x)
        image = image + prior_precision * total_sq * drift - jnp.sum(on_x, axis=1, keepdims=True) * current
        image = image / count
        if not last:
            moves[t, 1, 0] = image
            h_copies = send_dom(
                moves.at[t, 1, 0], lambda k: moves.at[t, 1, k], lambda k: h_send.at[t, k], lambda k: h_recv.at[t, k]
            )
            pending += h_copies
        exact = ahead(image)
        rough[t, 0] = exact.astype(bf16)
        c1 = send_dim(rough.at[t, 0], lambda k: rough.at[t, k], lambda k: r_send.at[t, k], lambda k: r_recv.at[t, k])
        image_sq = jnp.sum(image * image, axis=1, keepdims=True)
        marks = jnp.where(lane == 0, jnp.sum(drift * drift, axis=1, keepdims=True), 0.0)
        marks = jnp.where(lane == 1, jnp.sum(drift * image, axis=1, keepdims=True), marks)
        marks = jnp.where(lane == 2, image_sq, marks)
        marks = jnp.where(lane == 3, prior_precision * total_sq * image_sq, marks)
        marked[t, 0] = jnp.concatenate(
            [jnp.sum(marks, axis=0, keepdims=True), flat(exact[:, :draws]), jnp.zeros((rows - 2, LANES), f32)], axis=0
        )
        c2 = send_dim(marked.at[t, 0], lambda k: marked.at[t, k], lambda k: m_send.at[t, k], lambda k: m_recv.at[t, k])
        pending += c1 + c2
        if not last:
            for copy in b_copies + h_copies:
                copy.wait_recv()
            every = [everyone, moves[t, 0].reshape(count, width), moves[t, 1].reshape(count, width)]
            own = [current, drift, image]
            pairs = [(0, 1), (0, 2), (1, 1), (1, 2), (2, 2)]
            own_pieces = halves(jnp.concatenate(own, axis=0))
            inner = [paired(fold(dot_t(own_pieces, halves(v)))) for v in every]
            square = column_sums(jnp.concatenate([every[u] * every[v] for u, v in pairs], axis=0))
            terms = []
            for n, (u, v) in enumerate(pairs):
                mixed = inner[v][u * rows : (u + 1) * rows] + inner[u][v * rows : (v + 1) * rows]
                terms.append(row_sums(own[u] * own[v]) + square[:, n * count : (n + 1) * count] - mixed)
            spare = cross_terms.shape[-1] - len(pairs) * count
            if spare > 0:
                terms.append(jnp.zeros((rows, spare), f32))
            cross_terms[t, 0] = jnp.concatenate(terms, axis=1)
            g_copies = send_dim(
                cross_terms.at[t, 0], lambda k: cross_terms.at[t, k], lambda k: g_send.at[t, k], lambda k: g_recv.at[t, k]
            )
            pending += g_copies
        for copy in c1 + c2:
            copy.wait_recv()
        seen = functools.reduce(jnp.add, [rough[t, k].astype(f32) for k in range(1, nz)], exact)
        along = seen[:, cols : cols + count]
        gap = along - own_dots(along)
        bent = jnp.sum(weight * seen[:, :cols] * seen[:, :cols], axis=1, keepdims=True)
        bent = bent + cross * jnp.sum(kernel_sq * gap * gap, axis=1, keepdims=True)
        marks = functools.reduce(jnp.add, [marked[t, k] for k in range(nz)])
        bent = jnp.sum(bent, axis=0, keepdims=True)
        sums[t, 0] = jnp.concatenate(
            [marks[0:1] + jnp.where(lane[0:1] == 3, bent, 0.0), drift_logits, marks[1:2], marks[3:]], axis=0
        )
        copies = send_dom(
            sums.at[t, 0], lambda k: sums.at[t, k], lambda k: s_send.at[t, k], lambda k: s_recv.at[t, k]
        )
        pending += copies
        for copy in copies:
            copy.wait_recv()
        marks = functools.reduce(jnp.add, [sums[t, k, 0:1] for k in range(nd)])
        first = lax.broadcasted_iota(jnp.int32, (1, LANES), 1)
        norm, curve_total, image_square, bent = [
            jnp.sum(jnp.where(first == k, marks, 0.0), axis=1, keepdims=True) for k in range(4)
        ]
        bent = bent / count
        alpha = norm / curve_total
        norm_next = norm - 2.0 * alpha * curve_total + alpha * alpha * image_square
        keep = 1.0 + norm_next / norm
        curve_next = keep * keep * curve_total - 2.0 * keep * alpha * image_square + alpha * alpha * bent
        alpha_next = norm_next / curve_next
        on_drift, on_image = alpha + alpha_next * keep, -alpha_next * alpha
        update = on_drift * drift + on_image * image
        out_ref[t] = update
        if not last:
            current = current + move_size * update
            step_b, step_h = move_size * on_drift, move_size * on_image
            everyone = everyone + step_b * every[1] + step_h * every[2]
            basis[cols:, :] = halves(everyone)
            shifts = [sums[t, k, 1:2] * step_b + sums[t, k, 2:3] * step_h for k in range(nd)]
            logits = logits + jnp.concatenate(shifts, axis=0)
            for copy in g_copies:
                copy.wait_recv()
            terms = functools.reduce(jnp.add, [cross_terms[t, k] for k in range(nz)])
            by = [2.0 * step_b, 2.0 * step_h, step_b * step_b, 2.0 * step_b * step_h, step_h * step_h]
            for n, factor in enumerate(by):
                distance = distance + factor * terms[:, n * count : (n + 1) * count]
    for copy in pending:
        copy.wait_send()


def solution(mesh):
    nd, nz = mesh.shape["dom"], mesh.shape["dim"]

    def per_device(particles, data_rows, labels):
        rows, width = particles.shape
        draws = data_rows.shape[0] * data_rows.shape[1]
        count = nd * rows
        wide = -(-count // LANES) * LANES
        cols = nd * draws
        dma = pltpu.SemaphoreType.DMA
        over_dom, over_dim = (NEWTON, nd), (NEWTON, nz)
        pairs = [(nd,), (nd,), (nz,), (nz,)] + [over_dim] * 3 + [over_dom] * 3 + [over_dim]
        return pl.pallas_call(
            functools.partial(steps, nd, nz),
            out_shape=jax.ShapeDtypeStruct((NEWTON, rows, width), f32),
            in_specs=[pl.BlockSpec(memory_space=pltpu.VMEM)] * 3,
            out_specs=pl.BlockSpec(memory_space=pltpu.VMEM),
            scratch_shapes=[
                pltpu.VMEM((cols + 2 * count, width), bf16),
                pltpu.VMEM((count, cols), bf16),
                pltpu.VMEM((nd, rows, width + draws), f32),
                pltpu.VMEM((nz, rows, wide), f32),
                pltpu.VMEM((nz, nd, draws), f32),
                pltpu.VMEM((NEWTON, nz, rows, cols + wide), f32),
                pltpu.VMEM((NEWTON, nz, rows, cols + wide), bf16),
                pltpu.VMEM((NEWTON, nz, rows, LANES), f32),
                pltpu.VMEM((NEWTON, nd, rows, LANES), f32),
                pltpu.VMEM((NEWTON, 2, nd, rows, width), f32),
                pltpu.VMEM((NEWTON, nz, rows, -(-5 * count // LANES) * LANES), f32),
            ]
            + [dma(shape) for shape in pairs for _ in range(2)],
            compiler_params=pltpu.CompilerParams(collective_id=0, has_side_effects=True),
        )(particles, data_rows.reshape(draws, width), labels)

    placed = (P("dom", "dim"), P("dom", None, "dim"), P("dom", None))
    return jax.shard_map(
        per_device, mesh=mesh, in_specs=placed, out_specs=P(None, "dom", "dim"), check_vma=False
    )
```
